32 devices in a mesh: zero: 4 (over x, core), width: 8 (over z, y).
Axes of the slice: x: 2, y: 2, z: 4, core: 2. Of those that a mesh axis runs over, the one named last changes fastest.
Arguments:
- weight_query: float32 [8192, 8192], P('zero', 'width'), may hold values from -0.09375 to 0.09375
- smooth_query: float32 [8192, 8192], P('zero', 'width'), may hold values from -0.0625 to 0.0625
- weight_key: float32 [8192, 512], P('zero', 'width'), may hold values from -0.09375 to 0.09375
- smooth_key: float32 [8192, 512], P('zero', 'width'), may hold values from -0.0625 to 0.0625
- weight_value: float32 [8192, 512], P('zero', 'width'), may hold values from -0.09375 to 0.09375
- smooth_value: float32 [8192, 512], P('zero', 'width'), may hold values from -0.0625 to 0.0625
- norm_train: float32 [8192], P(('zero', 'width')), may hold values from 0.25 to 1.75
- norm_step: float32 [8192], P(('zero', 'width')), may hold values from -0.3 to 0.3
Outputs:
- final_query: bfloat16 [8192, 8192], P(None, 'width')
- final_key: bfloat16 [8192, 512], P(None, 'width')
- final_value: bfloat16 [8192, 512], P(None, 'width')
- factor_query: float32 [8192], P('width')
- factor_key: float32 [512], P('width')
- factor_value: float32 [512], P('width')
- serve_norm: bfloat16 [8192], replicated
- result_query: float32 [8192, 8192], P('zero', 'width')
- result_key: float32 [8192, 512], P('zero', 'width')
- result_value: float32 [8192, 512], P('zero', 'width')
The draws below stay inside these ranges and needn't reach their ends.
All inputs are finite; a program needn't handle non-finite values. Where the reference program divides by a largest or mean magnitude, that divisor is 1e-20 or more.
Results may differ from the reference program's by a relative error of at most 0.001.
Values may be sent and summed in bfloat16 or wider, within the bound.
A program may use at most 128 MiB of HBM per device.

```python
import jax
import jax.numpy as jnp

D_MODEL = 8192
Q_DIM = 8192
KV_DIM = 512


def with_spikes(array, stream_key, source, target, shards_of, factor):
    owner, partner = [(jnp.arange(array.shape[position]) // (array.shape[position] // shards_of)).reshape([-1 if axis == position else 1 for axis in range(array.ndim)]) for position in (source, target)]
    chosen = jax.random.permutation(stream_key, shards_of)[partner]
    strong = (owner == chosen) | (owner == (partner + shards_of // 2) % shards_of)
    return jnp.where(strong, factor * array, array)


def block_scale(own_key, dims, shards, least, high):
    level, own = 1.0, jax.random.fold_in(own_key, 6)
    for axis_at, shards_of in shards:
        draws = jnp.exp(jax.random.uniform(jax.random.fold_in(own, axis_at), (shards_of,), jnp.float32, least / len(shards), high / len(shards)))
        level = level * jnp.repeat(draws, dims[axis_at] // shards_of).reshape([-1 if axis == axis_at else 1 for axis in range(len(dims))])
    return level


def normal_values(stream_key, extent, spread, limit, pieces=(), dtype=jnp.bfloat16):
    values = jax.random.normal(stream_key, extent, jnp.float32) * spread
    if len(pieces) > 0:
        values = block_scale(stream_key, extent, pieces, -0.22, 0.18) * values
    return jnp.clip(values, min=-limit, max=limit).astype(dtype)


def gaussian_with(rng, shape, width, most, cuts, heavy, kind=jnp.bfloat16):
    drawn = width * jax.random.normal(rng, shape, jnp.float32)
    if cuts:
        drawn = drawn * block_scale(rng, shape, cuts, -0.22, 0.18)
    return jnp.clip(with_spikes(drawn, jax.random.fold_in(rng, 3), *heavy), -most, most).astype(kind)


def setup_inputs(seed: int = 0) -> dict:
    key_list = jax.random.split(jax.random.key(seed), 9)
    return {
        "weight_query": gaussian_with(key_list[0], (D_MODEL, Q_DIM), D_MODEL ** -0.5, 0.09375, ((0, 4), (1, 8)), (0, 1, 8, 2.0), jnp.float32),
        "smooth_query": normal_values(key_list[1], (D_MODEL, Q_DIM), D_MODEL ** -0.5, 0.0625, ((0, 4), (1, 8)), jnp.float32),
        "weight_key": gaussian_with(key_list[2], (D_MODEL, KV_DIM), D_MODEL ** -0.5, 0.09375, ((0, 4), (1, 8)), (0, 1, 8, 2.0), jnp.float32),
        "smooth_key": normal_values(key_list[3], (D_MODEL, KV_DIM), D_MODEL ** -0.5, 0.0625, ((0, 4), (1, 8)), jnp.float32),
        "weight_value": gaussian_with(key_list[4], (D_MODEL, KV_DIM), D_MODEL ** -0.5, 0.09375, ((0, 4), (1, 8)), (0, 1, 8, 2.0), jnp.float32),
        "smooth_value": normal_values(key_list[5], (D_MODEL, KV_DIM), D_MODEL ** -0.5, 0.0625, ((0, 4), (1, 8)), jnp.float32),
        "norm_train": jnp.clip(1.0 + 0.15 * jax.random.normal(key_list[6], (D_MODEL,), jnp.float32), 0.25, 1.75),
        "norm_step": jnp.clip(jax.random.uniform(key_list[7], (D_MODEL,), jnp.float32, -0.3, 0.3) * block_scale(key_list[7], (D_MODEL,), ((0, 32),), -0.4, 0.0), -0.3, 0.3),
    }


keep_rate = 0.7


def reference(weight_query, smooth_query, weight_key, smooth_key, weight_value, smooth_value, norm_train, norm_step):
    result_query = keep_rate * smooth_query + (1.0 - keep_rate) * weight_query
    result_key = keep_rate * smooth_key + (1.0 - keep_rate) * weight_key
    result_value = keep_rate * smooth_value + (1.0 - keep_rate) * weight_value
    factor_query = jnp.sum(jnp.abs(result_query), axis=0) / D_MODEL
    final_query = (result_query / factor_query).astype(jnp.bfloat16)
    factor_key = jnp.sum(jnp.abs(result_key), axis=0) / D_MODEL
    final_key = (result_key / factor_key).astype(jnp.bfloat16)
    factor_value = jnp.sum(jnp.abs(result_value), axis=0) / D_MODEL
    final_value = (result_value / factor_value).astype(jnp.bfloat16)
    serve_norm = (norm_train + norm_step).astype(jnp.bfloat16)
    return final_query, final_key, final_value, factor_query, factor_key, factor_value, serve_norm, result_query, result_key, result_value
```

```python
import functools

import jax
import jax.numpy as jnp
from jax import lax
from jax.experimental import pallas as pl
from jax.experimental.pallas import tpu as pltpu
from jax.sharding import PartitionSpec as P

keep_rate = 0.7
CORES = 2
STEP = 16
PARTS = (0.35, 0.30, 0.20, 0.11, 0.04)
MESH = pl.DeviceIdType.MESH


def blend(smooth, weight):
    return keep_rate * smooth + (1.0 - keep_rate) * weight


def heights_of(rows):
    cuts = [0]
    done = 0.0
    for part in PARTS[:-1]:
        done += part
        cuts.append(int(rows * done) // 64 * 64)
    cuts.append(rows)
    return [b - a for a, b in zip(cuts, cuts[1:])]


def head_kernel(zeros, heights, blocks, *refs):
    wq, sq, wk, sk, wv, sv = refs[:6]
    count = len(heights)
    narrow_out = refs[6 : 6 + count]
    kv_out, factor = refs[6 + count : 8 + count]
    (vwq, vsq, vw, vs, narrow, narrow_kv, sums, got,
     in_sem, small_sem, out_sem, send_sem, recv_sem) = refs[8 + count :]
    rows, wide = wq.shape
    small = wk.shape[0]
    both = 2 * small
    block = rows // blocks
    me = lax.axis_index("zero")

    smalls = [
        pltpu.make_async_copy(src, dst, small_sem.at[i])
        for i, (src, dst) in enumerate((
            (wk, vw.at[pl.ds(0, small)]), (sk, vs.at[pl.ds(0, small)]),
            (wv, vw.at[pl.ds(small, small)]), (sv, vs.at[pl.ds(small, small)]),
        ))
    ]
    for copy in smalls:
        copy.start()
    copies = []
    for b in range(blocks):
        at = pl.ds(b * block, block)
        pair = (
            pltpu.make_async_copy(wq.at[at], vwq.at[at], in_sem.at[0, b]),
            pltpu.make_async_copy(sq.at[at], vsq.at[at], in_sem.at[1, b]),
        )
        for copy in pair:
            copy.start()
        copies.append(pair)
    barrier = pltpu.get_barrier_semaphore()
    for k in range(1, zeros):
        pl.semaphore_signal(
            barrier, inc=1, device_id={"zero": lax.rem(me + k, zeros)}, device_id_type=MESH
        )

    for copy in smalls:
        copy.wait()

    def add_small(i, acc):
        at = pl.ds(pl.multiple_of(i * 128, 128), 128)
        value = blend(vs[:, at], vw[:, at])
        vw[:, at] = value
        return acc + jnp.abs(value)

    total_kv = lax.fori_loop(0, rows // 128, add_small, jnp.zeros((both, 128), jnp.float32))
    sums[:, wide : wide + both] = jnp.sum(total_kv.T, axis=0, keepdims=True)

    total_q = jnp.zeros((8, wide), jnp.float32)
    for b in range(blocks):
        for copy in copies[b]:
            copy.wait()

        def add(i, acc, b=b):
            at = pl.ds(pl.multiple_of(b * block + i * STEP, STEP), STEP)
            value = blend(vsq[at, :], vwq[at, :])
            vwq[at, :] = value
            size = jnp.abs(value)
            for r in range(0, STEP, 8):
                acc = acc + size[r : r + 8]
            return acc

        total_q = lax.fori_loop(0, block // STEP, add, total_q)
    sums[:, 0:wide] = jnp.sum(total_q, axis=0, keepdims=True)

    pl.semaphore_wait(barrier, zeros - 1)
    sends = []
    for k in range(1, zeros):
        send = pltpu.make_async_remote_copy(
            src_ref=sums, dst_ref=got.at[k - 1],
            send_sem=send_sem.at[k - 1], recv_sem=recv_sem.at[k - 1],
            device_id={"zero": lax.rem(me + k, zeros)}, device_id_type=MESH,
        )
        send.start()
        sends.append(send)
    for send in sends:
        send.wait()
    total = sums[...]
    for k in range(zeros - 1):
        total = total + got[k]
    scale = total / (rows * zeros)
    factor[...] = scale
    back = 1.0 / scale
    back_q = back[:, 0:wide]
    back_kv = jnp.broadcast_to(back[:, wide : wide + both], (128, both)).T

    def scale_small(i, carry):
        at = pl.ds(pl.multiple_of(i * 128, 128), 128)
        narrow_kv[:, at] = (vw[:, at] * back_kv).astype(jnp.bfloat16)
        return carry

    outs = []
    first = 0
    for n, height in enumerate(heights):

        def scale_rows(i, carry, first=first):
            at = pl.ds(pl.multiple_of(first + i * STEP, STEP), STEP)
            narrow[at, :] = (vwq[at, :] * back_q).astype(jnp.bfloat16)
            return carry

        lax.fori_loop(0, height // STEP, scale_rows, 0)
        out = pltpu.make_async_copy(
            narrow.at[pl.ds(first, height)], narrow_out[n], out_sem.at[n]
        )
        out.start()
        outs.append(out)
        first += height
    lax.fori_loop(0, rows // 128, scale_small, 0)
    out = pltpu.make_async_copy(narrow_kv, kv_out, out_sem.at[count])
    out.start()
    outs.append(out)
    for out in outs:
        out.wait()


def head(zeros, heights, wq, sq, wk, sk, wv, sv):
    rows, wide = wq.shape
    both = 2 * wk.shape[0]
    blocks = 8
    f32, bf16 = jnp.float32, jnp.bfloat16
    return pl.pallas_call(
        functools.partial(head_kernel, zeros, heights, blocks),
        out_shape=[jax.ShapeDtypeStruct((h, wide), bf16) for h in heights]
        + [jax.ShapeDtypeStruct((both, rows), bf16), jax.ShapeDtypeStruct((1, wide + both), f32)],
        in_specs=[pl.BlockSpec(memory_space=pl.ANY)] * 6,
        out_specs=[pl.BlockSpec(memory_space=pl.ANY)] * (len(heights) + 1)
        + [pl.BlockSpec(memory_space=pltpu.VMEM)],
        scratch_shapes=[
            pltpu.VMEM((rows, wide), f32), pltpu.VMEM((rows, wide), f32),
            pltpu.VMEM((both, rows), f32), pltpu.VMEM((both, rows), f32),
            pltpu.VMEM((rows, wide), bf16), pltpu.VMEM((both, rows), bf16),
            pltpu.VMEM((1, wide + both), f32), pltpu.VMEM((zeros - 1, 1, wide + both), f32),
            pltpu.SemaphoreType.DMA((2, blocks)),
            pltpu.SemaphoreType.DMA((4,)),
            pltpu.SemaphoreType.DMA((len(heights) + 1,)),
            pltpu.SemaphoreType.DMA((zeros - 1,)),
            pltpu.SemaphoreType.DMA((zeros - 1,)),
        ],
        compiler_params=pltpu.CompilerParams(
            collective_id=0, has_side_effects=True, vmem_limit_bytes=60 * 2**20
        ),
        cost_estimate=pl.CostEstimate(
            flops=6 * rows * wide, bytes_accessed=12 * rows * wide, transcendentals=0
        ),
    )(wq, sq, wk, sk, wv, sv)


def norm_kernel(zeros, widths, train, step, out, mine, all_of, send_sem, recv_sem):
    count = zeros * widths
    me_zero, me_width = lax.axis_index("zero"), lax.axis_index("width")
    me = me_zero * widths + me_width
    barrier = pltpu.get_barrier_semaphore()

    def place(k):
        other = lax.rem(me + k, count)
        return {"zero": other // widths, "width": lax.rem(other, widths)}

    def greet(k, carry):
        pl.semaphore_signal(barrier, inc=1, device_id=place(k), device_id_type=MESH)
        return carry

    lax.fori_loop(1, count, greet, 0)
    mine[...] = train[...] + step[...]
    pl.semaphore_wait(barrier, count - 1)

    def copy(k):
        return pltpu.make_async_remote_copy(
            src_ref=mine, dst_ref=all_of.at[k],
            send_sem=send_sem.at[k], recv_sem=recv_sem.at[k],
            device_id=place(k), device_id_type=MESH,
        )

    def send(k, carry):
        copy(k).start()
        return carry

    lax.fori_loop(1, count, send, 0)
    out[me] = mine[...]

    def take(k, carry):
        copy(k).wait()
        out[lax.rem(me + count - k, count)] = all_of[k]
        return carry

    lax.fori_loop(1, count, take, 0)


def norm_gather(zeros, widths, train, step):
    count = zeros * widths
    size = train.shape[0]
    f32 = jnp.float32
    return pl.pallas_call(
        functools.partial(norm_kernel, zeros, widths),
        out_shape=jax.ShapeDtypeStruct((count, 1, size), f32),
        in_specs=[pl.BlockSpec(memory_space=pltpu.VMEM)] * 2,
        out_specs=pl.BlockSpec(memory_space=pltpu.VMEM),
        scratch_shapes=[
            pltpu.VMEM((1, size), f32),
            pltpu.VMEM((count, 1, size), f32),
            pltpu.SemaphoreType.DMA((count,)),
            pltpu.SemaphoreType.DMA((count,)),
        ],
        compiler_params=pltpu.CompilerParams(collective_id=1, has_side_effects=True),
        cost_estimate=pl.CostEstimate(flops=0, bytes_accessed=2**23, transcendentals=0),
    )(train.reshape(1, size), step.reshape(1, size))


def place_kernel(chips, outs_of, old_count, *refs):
    count = chips * CORES
    pieces = refs[:count]
    outs = refs[count + old_count : -3]
    buf, in_sem, out_sem = refs[-3:]
    me = lax.axis_index("zero")
    chip, core = me // CORES, lax.rem(me, CORES)
    ins, sent = [], []
    for p in range(count):
        copy = pltpu.make_async_copy(pieces[p], buf.at[p], in_sem.at[p])
        copy.start()
        ins.append(copy)
    for p in range(count):
        back, swap = p // CORES, p % CORES
        owner = lax.rem(chip + chips - back, chips) * CORES + lax.rem(core + swap, CORES)
        ins[p].wait()
        for n, (src, dst) in enumerate(outs_of(buf.at[p], outs, owner)):
            copy = pltpu.make_async_copy(src, dst, out_sem.at[n, p])
            copy.start()
            sent.append(copy)
    for copy in sent:
        copy.wait()


def place(chips, outs_of, shapes, pieces, old):
    count = chips * CORES
    bf16 = jnp.bfloat16
    old = () if old is None else tuple(old)
    return pl.pallas_call(
        functools.partial(place_kernel, chips, outs_of, len(old)),
        out_shape=[jax.ShapeDtypeStruct(shape, bf16) for shape in shapes],
        in_specs=[pl.BlockSpec(memory_space=pl.ANY)] * (count + len(old)),
        out_specs=[pl.BlockSpec(memory_space=pl.ANY)] * len(shapes),
        input_output_aliases={count + n: n for n in range(len(old))},
        scratch_shapes=[
            pltpu.VMEM((count,) + pieces[0].shape, bf16),
            pltpu.SemaphoreType.DMA((count,)),
            pltpu.SemaphoreType.DMA((len(shapes), count)),
        ],
        compiler_params=pltpu.CompilerParams(
            vmem_limit_bytes=2 * count * pieces[0].size + 2**20
        ),
        cost_estimate=pl.CostEstimate(
            flops=0, bytes_accessed=4 * count * pieces[0].size, transcendentals=0
        ),
    )(*pieces, *old)


def on_device(zeros, widths, wq, sq, wk, sk, wv, sv, train, step):
    rows, wide = wq.shape
    small = wk.shape[1]
    chips = zeros // CORES
    heights = heights_of(rows)
    *narrow, narrow_kv, factor = head(zeros, heights, wq, sq, wk.T, sk.T, wv.T, sv.T)
    across = [
        [(x * CORES + c, (x + k) % chips * CORES + c) for x in range(chips) for c in range(CORES)]
        for k in range(chips)
    ]
    swap = [(x * CORES + c, x * CORES + (c + 1) % CORES) for x in range(chips) for c in range(CORES)]

    def arrive(block):
        got = [block]
        for k in range(1, chips):
            got.append(lax.ppermute(block, "zero", across[k]))
        return got

    def pieces_of(blocks):
        return [p for b in blocks for p in (b, lax.ppermute(b, "zero", swap))]

    kv_blocks = arrive(narrow_kv)
    arrived = [arrive(block) for block in narrow]
    result_q = blend(sq, wq)
    result_k, result_v = blend(sk, wk), blend(sv, wv)
    serve = norm_gather(zeros, widths, train, step)

    def columns_of(src, outs, owner):
        at = pl.ds(pl.multiple_of(owner * rows, 128), rows)
        return [(src.at[pl.ds(n * small, small)], outs[n].at[:, at]) for n in range(2)]

    kv_blocks, (result_q, result_k, result_v, serve) = lax.optimization_barrier(
        (kv_blocks, (result_q, result_k, result_v, serve))
    )
    final_kv = place(chips, columns_of, [(small, rows * zeros)] * 2, pieces_of(kv_blocks), None)
    arrived[0], final_kv = lax.optimization_barrier((arrived[0], final_kv))
    final = None
    first = 0
    for n, blocks in enumerate(arrived):
        if n:
            blocks, final = lax.optimization_barrier((blocks, final))
        height = blocks[0].shape[0]

        def rows_of(src, outs, owner, first=first, height=height):
            at = pl.ds(pl.multiple_of(owner * rows + first, 64), height)
            return [(src, outs[0].at[at])]

        final = place(chips, rows_of, [(rows * zeros, wide)], pieces_of(blocks), final)
        first += height
    factor = factor.reshape(-1)
    return (
        final[0],
        final_kv[0].T,
        final_kv[1].T,
        factor[:wide],
        factor[wide : wide + small],
        factor[wide + small :],
        serve.reshape(-1).astype(jnp.bfloat16),
        result_q,
        result_k,
        result_v,
    )


def solution(mesh):
    grid = P("zero", "width")
    in_specs = (grid,) * 6 + (P(("zero", "width")),) * 2
    out_specs = (
        (P(None, "width"),) * 3 + (P("width"),) * 3 + (P(),) + (grid,) * 3
    )
    zeros, widths = mesh.shape["zero"], mesh.shape["width"]

    def whole(*args):
        return on_device(zeros, widths, *args)

    return jax.shard_map(
        whole, mesh=mesh, in_specs=in_specs, out_specs=out_specs, check_vma=False
    )
```

```python
import functools

import jax
import jax.numpy as jnp
from jax import lax
from jax.experimental import pallas as pl
from jax.experimental.pallas import tpu as pltpu
from jax.sharding import PartitionSpec as P

keep_rate = 0.7
CORES = 2
STEP = 16
PARTS = (0.25, 0.29, 0.25, 0.15, 0.06)
MESH = pl.DeviceIdType.MESH


def blend(smooth, weight):
    return keep_rate * smooth + (1.0 - keep_rate) * weight


def heights_of(rows):
    cuts = [0]
    done = 0.0
    for part in PARTS[:-1]:
        done += part
        cuts.append(int(rows * done) // 64 * 64)
    cuts.append(rows)
    return [b - a for a, b in zip(cuts, cuts[1:])]


def head_kernel(zeros, widths, blocks, *refs):
    wq, sq, wk, sk, wv, sv, train, step = refs[:8]
    kv_out, factor, norm = refs[8:11]
    (vwq, vsq, vw, vs, sums, got, mine, norms,
     in_sem, small_sem, send_sem, recv_sem, norm_send, norm_recv) = refs[11:]
    rows, wide = wq.shape
    small = wk.shape[0]
    both = 2 * small
    block = rows // blocks
    devices = zeros * widths
    me = lax.axis_index("zero")
    spot = me * widths + lax.axis_index("width")

    def there(k):
        other = lax.rem(spot + k, devices)
        return {"zero": other // widths, "width": lax.rem(other, widths)}

    smalls = [
        pltpu.make_async_copy(src, dst, small_sem.at[i])
        for i, (src, dst) in enumerate((
            (wk, vw.at[pl.ds(0, small)]), (sk, vs.at[pl.ds(0, small)]),
            (wv, vw.at[pl.ds(small, small)]), (sv, vs.at[pl.ds(small, small)]),
        ))
    ]
    for copy in smalls:
        copy.start()
    copies = []
    for b in range(blocks):
        at = pl.ds(b * block, block)
        pair = (
            pltpu.make_async_copy(wq.at[at], vwq.at[at], in_sem.at[0, b]),
            pltpu.make_async_copy(sq.at[at], vsq.at[at], in_sem.at[1, b]),
        )
        for copy in pair:
            copy.start()
        copies.append(pair)
    barrier = pltpu.get_barrier_semaphore()

    def greet(k, carry):
        pl.semaphore_signal(barrier, inc=1, device_id=there(k), device_id_type=MESH)
        return carry

    lax.fori_loop(1, devices, greet, 0)
    mine[...] = train[...] + step[...]

    for copy in smalls:
        copy.wait()

    def add_small(i, acc):
        at = pl.ds(pl.multiple_of(i * 128, 128), 128)
        value = blend(vs[:, at], vw[:, at])
        vw[:, at] = value
        return acc + jnp.abs(value)

    total_kv = lax.fori_loop(0, rows // 128, add_small, jnp.zeros((both, 128), jnp.float32))
    sums[:, wide : wide + both] = jnp.sum(total_kv.T, axis=0, keepdims=True)

    def norm_copy(k):
        return pltpu.make_async_remote_copy(
            src_ref=mine, dst_ref=norms.at[k],
            send_sem=norm_send.at[k], recv_sem=norm_recv.at[k],
            device_id=there(k), device_id_type=MESH,
        )

    def norm_start(k, carry):
        norm_copy(k).start()
        return carry

    total_q = jnp.zeros((8, wide), jnp.float32)
    for b in range(blocks):
        if b == blocks // 2:
            pl.semaphore_wait(barrier, devices - 1)
            lax.fori_loop(1, devices, norm_start, 0)
        for copy in copies[b]:
            copy.wait()

        def add(i, acc, b=b):
            at = pl.ds(pl.multiple_of(b * block + i * STEP, STEP), STEP)
            size = jnp.abs(blend(vsq[at, :], vwq[at, :]))
            for r in range(0, STEP, 8):
                acc = acc + size[r : r + 8]
            return acc

        total_q = lax.fori_loop(0, block // STEP, add, total_q, unroll=2)
    sums[:, 0:wide] = jnp.sum(total_q, axis=0, keepdims=True)

    sends = []
    for k in range(1, zeros):
        send = pltpu.make_async_remote_copy(
            src_ref=sums, dst_ref=got.at[k - 1],
            send_sem=send_sem.at[k - 1], recv_sem=recv_sem.at[k - 1],
            device_id={"zero": lax.rem(me + k, zeros)}, device_id_type=MESH,
        )
        send.start()
        sends.append(send)

    norm[spot] = mine[...]
    for send in sends:
        send.wait()
    total = sums[...]
    for k in range(zeros - 1):
        total = total + got[k]
    scale = total / (rows * zeros)
    factor[...] = scale
    back = 1.0 / scale[:, wide : wide + both]
    back_kv = jnp.broadcast_to(back, (128, both)).T

    def scale_small(i, carry):
        at = pl.ds(pl.multiple_of(i * 128, 128), 128)
        kv_out[:, at] = (vw[:, at] * back_kv).astype(jnp.bfloat16)
        return carry

    lax.fori_loop(0, rows // 128, scale_small, 0)

    def norm_take(k, carry):
        norm_copy(k).wait()
        norm[lax.rem(spot + devices - k, devices)] = norms[k]
        return carry

    lax.fori_loop(1, devices, norm_take, 0)


def head(zeros, widths, wq, sq, wk, sk, wv, sv, train, step):
    rows, wide = wq.shape
    both = 2 * wk.shape[0]
    size = train.shape[0]
    devices = zeros * widths
    blocks = 8
    f32, bf16 = jnp.float32, jnp.bfloat16
    return pl.pallas_call(
        functools.partial(head_kernel, zeros, widths, blocks),
        out_shape=[
            jax.ShapeDtypeStruct((both, rows), bf16),
            jax.ShapeDtypeStruct((1, wide + both), f32),
            jax.ShapeDtypeStruct((devices, 1, size), f32),
        ],
        in_specs=[pl.BlockSpec(memory_space=pl.ANY)] * 6
        + [pl.BlockSpec(memory_space=pltpu.VMEM)] * 2,
        out_specs=[pl.BlockSpec(memory_space=pltpu.VMEM)] * 3,
        scratch_shapes=[
            pltpu.VMEM((rows, wide), f32), pltpu.VMEM((rows, wide), f32),
            pltpu.VMEM((both, rows), f32), pltpu.VMEM((both, rows), f32),
            pltpu.VMEM((1, wide + both), f32), pltpu.VMEM((zeros - 1, 1, wide + both), f32),
            pltpu.VMEM((1, size), f32), pltpu.VMEM((devices, 1, size), f32),
            pltpu.SemaphoreType.DMA((2, blocks)),
            pltpu.SemaphoreType.DMA((4,)),
            pltpu.SemaphoreType.DMA((zeros - 1,)),
            pltpu.SemaphoreType.DMA((zeros - 1,)),
            pltpu.SemaphoreType.DMA((devices,)),
            pltpu.SemaphoreType.DMA((devices,)),
        ],
        compiler_params=pltpu.CompilerParams(
            collective_id=0, has_side_effects=True, vmem_limit_bytes=60 * 2**20
        ),
        cost_estimate=pl.CostEstimate(
            flops=6 * rows * wide, bytes_accessed=8 * rows * wide, transcendentals=0
        ),
    )(wq, sq, wk, sk, wv, sv, train.reshape(1, size), step.reshape(1, size))


def place_kernel(chips, outs_of, old_count, *refs):
    count = chips * CORES
    pieces = refs[:count]
    outs = refs[count + old_count : -3]
    buf, in_sem, out_sem = refs[-3:]
    me = lax.axis_index("zero")
    chip, core = me // CORES, lax.rem(me, CORES)
    ins, sent = [], []
    for p in range(count):
        copy = pltpu.make_async_copy(pieces[p], buf.at[p], in_sem.at[p])
        copy.start()
        ins.append(copy)
    for p in range(count):
        back, swap = p // CORES, p % CORES
        owner = lax.rem(chip + chips - back, chips) * CORES + lax.rem(core + swap, CORES)
        ins[p].wait()
        for n, (src, dst) in enumerate(outs_of(buf.at[p], outs, owner)):
            copy = pltpu.make_async_copy(src, dst, out_sem.at[n, p])
            copy.start()
            sent.append(copy)
    for copy in sent:
        copy.wait()


def place(chips, outs_of, shapes, pieces, old):
    count = chips * CORES
    bf16 = jnp.bfloat16
    old = () if old is None else tuple(old)
    return pl.pallas_call(
        functools.partial(place_kernel, chips, outs_of, len(old)),
        out_shape=[jax.ShapeDtypeStruct(shape, bf16) for shape in shapes],
        in_specs=[pl.BlockSpec(memory_space=pl.ANY)] * (count + len(old)),
        out_specs=[pl.BlockSpec(memory_space=pl.ANY)] * len(shapes),
        input_output_aliases={count + n: n for n in range(len(old))},
        scratch_shapes=[
            pltpu.VMEM((count,) + pieces[0].shape, bf16),
            pltpu.SemaphoreType.DMA((count,)),
            pltpu.SemaphoreType.DMA((len(shapes), count)),
        ],
        compiler_params=pltpu.CompilerParams(
            vmem_limit_bytes=2 * count * pieces[0].size + 2**20
        ),
        cost_estimate=pl.CostEstimate(
            flops=0, bytes_accessed=4 * count * pieces[0].size, transcendentals=0
        ),
    )(*pieces, *old)


def on_device(zeros, widths, wq, sq, wk, sk, wv, sv, train, step):
    rows, wide = wq.shape
    small = wk.shape[1]
    chips = zeros // CORES
    heights = heights_of(rows)
    narrow_kv, factor, serve = head(
        zeros, widths, wq, sq, wk.T, sk.T, wv.T, sv.T, train, step
    )
    narrow = []
    first = 0
    for height in heights:
        at = slice(first, first + height)
        narrow.append((blend(sq[at], wq[at]) / factor[:, :wide]).astype(jnp.bfloat16))
        first += height
    across = [
        [(x * CORES + c, (x + k) % chips * CORES + c) for x in range(chips) for c in range(CORES)]
        for k in range(chips)
    ]
    swap = [(x * CORES + c, x * CORES + (c + 1) % CORES) for x in range(chips) for c in range(CORES)]

    def arrive(block):
        got = [block]
        for k in range(1, chips):
            got.append(lax.ppermute(block, "zero", across[k]))
        return got

    def pieces_of(blocks):
        return [p for b in blocks for p in (b, lax.ppermute(b, "zero", swap))]

    kv_blocks = arrive(narrow_kv)
    arrived = [arrive(block) for block in narrow]
    result_q = blend(sq, wq)
    result_k, result_v = blend(sk, wk), blend(sv, wv)

    def columns_of(src, outs, owner):
        at = pl.ds(pl.multiple_of(owner * rows, 128), rows)
        return [(src.at[pl.ds(n * small, small)], outs[n].at[:, at]) for n in range(2)]

    kv_blocks, (result_q, result_k, result_v) = lax.optimization_barrier(
        (kv_blocks, (result_q, result_k, result_v))
    )
    final_kv = place(chips, columns_of, [(small, rows * zeros)] * 2, pieces_of(kv_blocks), None)
    arrived[0], final_kv = lax.optimization_barrier((arrived[0], final_kv))
    final = None
    first = 0
    for n, blocks in enumerate(arrived):
        if n:
            blocks, final = lax.optimization_barrier((blocks, final))
        height = blocks[0].shape[0]

        def rows_of(src, outs, owner, first=first, height=height):
            at = pl.ds(pl.multiple_of(owner * rows + first, 64), height)
            return [(src, outs[0].at[at])]

        final = place(chips, rows_of, [(rows * zeros, wide)], pieces_of(blocks), final)
        first += height
    factor = factor.reshape(-1)
    return (
        final[0],
        final_kv[0].T,
        final_kv[1].T,
        factor[:wide],
        factor[wide : wide + small],
        factor[wide + small :],
        serve.reshape(-1).astype(jnp.bfloat16),
        result_q,
        result_k,
        result_v,
    )


def solution(mesh):
    grid = P("zero", "width")
    in_specs = (grid,) * 6 + (P(("zero", "width")),) * 2
    out_specs = (
        (P(None, "width"),) * 3 + (P("width"),) * 3 + (P(),) + (grid,) * 3
    )
    zeros, widths = mesh.shape["zero"], mesh.shape["width"]

    def whole(*args):
        return on_device(zeros, widths, *args)

    return jax.shard_map(
        whole, mesh=mesh, in_specs=in_specs, out_specs=out_specs, check_vma=False
    )
```
